32 devices in a mesh: gx: 4 (over z), gy: 4 (over y, x), gz: 2 (over core).
Axes of the slice: x: 2, y: 2, z: 4, core: 2. Of those that a mesh axis runs over, the one named last changes fastest.
Arguments:
- coarse_field: float32 [3, 128, 128, 512], P(None, 'gx', 'gy', 'gz'), may hold values from -6 to 6
- fine_field: float32 [3, 128, 16, 256], P(None, ('gx', 'gy', 'gz')), may hold values from -6 to 6
- viscosity: float32 [128, 16, 256], P(('gx', 'gy', 'gz')), may hold values from 0.1 to 1
- corners: int32 [64, 3], replicated, may hold values from 0 to 504, as said below
- grid_slot: int32 [64], replicated, may hold values from 0 to 127, as said below
- neighbors: int32 [64, 2], replicated, may hold values from -1 to 63, as said below
Outputs:
- fine_out: float32 [3, 128, 16, 256], P(None, ('gx', 'gy', 'gz'))
- coarse_out: float32 [3, 128, 128, 512], P(None, 'gx', 'gy', 'gz')
The draws below stay inside these ranges and needn't reach their ends.
Inputs may be any that keep to these rules, and one draw needn't show every extreme that they name: Each box is 8 coarse cells on a side, its corner coordinates are multiples of 8, it lies inside the domain and inside one coarse brick of 32 x 32 x 256 cells, and different grids have different boxes. A brick holds either no box or exactly 4 boxes, which share their y and z corners and are grids of one wake. `grid_slot`: different grids have different slots. A grid's slot lies on a device with the same gz index as the brick that holds its box. Every device holds at most 4 grids, some device holds 4 grids in every draw, and all grids of one device lie in one brick. `neighbors`: entry 0 is the grid of the same wake whose box touches the grid's lower x face, entry 1 the one touching its upper x face, or -1 where there is none.
All inputs are finite; a program needn't handle non-finite values.
Results may differ from the reference program's by a relative error of at most 0.00005.
Values sent between devices are 32-bit elements; how exact they have to be, the bound alone decides.
A program may use at most 128 MiB of HBM per device.

```python
import math
import jax
import jax.numpy as jnp
from jax import lax

B = 8
F = 16
CY = 32
CZ = 256
SLOTS = 4
WAKE = 8
NX = 128
NY = 128
NZ = 512
N_GX = 4
N_GY = 4
N_GZ = 2


def wind_layout(key):
    root_random_key = jax.random.fold_in(key, 4242)
    groups = N_GX * N_GY
    turbines = groups // 4
    half_x = N_GX // 2
    pair_count = groups // 2
    rows_z = CZ // B
    grid_count = turbines * WAKE
    corner_parts = []
    slot_parts = []
    near_parts = []
    for z_layer in range(N_GZ):
        subkeys = jax.random.split(jax.random.fold_in(root_random_key, z_layer), 7)
        pair_order = jax.random.permutation(subkeys[0], pair_count).astype(jnp.int32)
        first_pair = jax.random.randint(subkeys[1], (), half_x, pair_count, dtype=jnp.int32)
        found_at = jnp.argmax(pair_order == first_pair).astype(jnp.int32)
        pair_order = pair_order.at[found_at].set(pair_order[0]).at[0].set(first_pair)
        chosen = pair_order[:turbines]
        brick_row = chosen // half_x
        brick_first = 2 * (chosen % half_x)
        edge_z = rows_z - 1 if z_layer % 2 == 0 else 0
        inner_y = jax.random.randint(subkeys[2], (turbines,), 0, CY // B, dtype=jnp.int32).at[0].set(0)
        inner_z = jax.random.randint(subkeys[5], (turbines,), 0, rows_z, dtype=jnp.int32).at[0].set(edge_z)
        row_y = brick_row * (CY // B) + inner_y
        row_z = inner_z + z_layer * rows_z
        start_x = brick_first * SLOTS
        along_wake = jnp.arange(WAKE, dtype=jnp.int32)
        lattice_x = (start_x[:, None] + along_wake[None, :]).reshape(-1)
        lattice_y = jnp.repeat(row_y, WAKE)
        lattice_z = jnp.repeat(row_z, WAKE)
        corner_parts.append((jnp.stack([lattice_x, lattice_y, lattice_z], axis=1) * B).astype(jnp.int32))
        local_ids = jnp.arange(grid_count, dtype=jnp.int32)
        global_ids = local_ids + z_layer * grid_count
        in_wake = local_ids % WAKE
        near_parts.append(jnp.stack([jnp.where(in_wake > 0, global_ids - 1, -1), jnp.where(in_wake < WAKE - 1, global_ids + 1, -1)], axis=1).astype(jnp.int32))
        devices = jax.random.permutation(subkeys[3], groups).astype(jnp.int32)
        across = (devices[0] + groups // 2) % groups
        across_at = jnp.argmax(devices == across).astype(jnp.int32)
        devices = devices.at[across_at].set(devices[2]).at[2].set(across)
        second_share = jax.random.randint(subkeys[6], (), 1, SLOTS + 1, dtype=jnp.int32)
        shares = jax.random.randint(subkeys[4], (groups // 2,), 0, SLOTS + 1, dtype=jnp.int32).at[0].set(SLOTS).at[1].set(second_share)
        half_id = local_ids // SLOTS
        inside = local_ids % SLOTS
        share_limit = shares[half_id]
        owner_group = jnp.where(inside < share_limit, devices[2 * half_id], devices[2 * half_id + 1])
        owner_slot = jnp.where(inside < share_limit, inside, inside - share_limit)
        slot_parts.append(((owner_group * N_GZ + z_layer) * SLOTS + owner_slot).astype(jnp.int32))
    corner_table = jnp.concatenate(corner_parts, axis=0)
    slot_table = jnp.concatenate(slot_parts, axis=0)
    near_all = jnp.concatenate(near_parts, axis=0)
    total_count = corner_table.shape[0]
    renumbered_slots = jax.random.permutation(jax.random.fold_in(root_random_key, 777), total_count).astype(jnp.int32)
    inverse_permutation = jnp.argsort(renumbered_slots).astype(jnp.int32)
    mapped_neighbor_slots = jnp.where(near_all >= 0, inverse_permutation[jnp.maximum(near_all, 0)], -1).astype(jnp.int32)
    return (corner_table[renumbered_slots], slot_table[renumbered_slots], mapped_neighbor_slots[renumbered_slots])


def draw_corners(key, part):
    return wind_layout(key)[0]


def draw_grid_slot(key, part):
    return wind_layout(key)[1]


def draw_neighbors(key, part):
    return wind_layout(key)[2]


def steps_of(key, dims, pieces, least, high):
    def one(axis_at, shards_of):
        heights = jax.random.uniform(jax.random.fold_in(jax.random.fold_in(key, 6), axis_at), (shards_of,), jnp.float32, least / len(pieces), high / len(pieces))
        return jnp.repeat(jnp.exp(heights), dims[axis_at] // shards_of).reshape((-1,) + (1,) * (len(dims) - axis_at - 1))

    factor_of = one(*pieces[0])
    for cut in pieces[1:]:
        factor_of = factor_of * one(*cut)
    return factor_of


def centred(own_key, shape, scale, reach, pieces=(), held_as=jnp.bfloat16):
    result = scale * jax.random.normal(own_key, shape, jnp.float32)
    if pieces:
        result = result * steps_of(own_key, shape, pieces, -0.22, 0.18)
    return jnp.clip(result, -reach, reach).astype(held_as)


def setup_inputs(seed: int = 0) -> dict:
    keys = jax.random.split(jax.random.key(seed), 7)
    return {
        "coarse_field": centred(keys[0], (3, NX, NY, NZ), 1.0, 6.0, ((1, 4), (2, 4), (3, 2)), jnp.float32),
        "fine_field": centred(keys[1], (3, N_GX * N_GY * N_GZ * SLOTS, F, F * F), 1.0, 6.0, ((1, 32),), jnp.float32),
        "viscosity": jnp.clip(jnp.exp(math.log(1.0) - 2.3025851 * jax.random.uniform(keys[2], (N_GX * N_GY * N_GZ * SLOTS, F, F * F), jnp.float32) ** steps_of(keys[2], (N_GX * N_GY * N_GZ * SLOTS, F, F * F), ((0, 32),), -0.2, 0.2)), 0.1, 1.0),
        "corners": draw_corners(jax.random.fold_in(keys[6], 71), 0),
        "grid_slot": draw_grid_slot(jax.random.fold_in(keys[6], 71), 0),
        "neighbors": draw_neighbors(jax.random.fold_in(keys[6], 71), 0),
    }


step_rate = 0.15


def tables():
    side = B + 2
    fine_index = jnp.arange(F, dtype=jnp.int32)
    coarse_index = jnp.arange(side, dtype=jnp.int32)
    center = fine_index // 2 + 1
    other = jnp.where(fine_index % 2 == 0, center - 1, center + 1)
    tangent = 0.75 * (coarse_index[None, :] == center[:, None]).astype(jnp.float32) + 0.25 * (coarse_index[None, :] == other[:, None]).astype(jnp.float32)
    low_side = 0.75 * (coarse_index == 0).astype(jnp.float32) + 0.25 * (coarse_index == 1).astype(jnp.float32)
    high_side = 0.75 * (coarse_index == side - 1).astype(jnp.float32) + 0.25 * (coarse_index == side - 2).astype(jnp.float32)
    return tangent, low_side, high_side


def advance(volume, visc_cells, ghost_faces, lower_plane, upper_plane):
    components = volume.shape[0]
    slots_here = volume.shape[1]
    cells_edge = volume.shape[2]
    plane_size = volume.shape[3]
    lane_ids = jnp.arange(plane_size, dtype=jnp.int32)
    lane_y = lane_ids // cells_edge
    lane_z = lane_ids % cells_edge
    x_minus = jnp.concatenate([lower_plane[:, :, None], volume[:, :, :-1]], axis=2)
    x_plus = jnp.concatenate([volume[:, :, 1:], upper_plane[:, :, None]], axis=2)
    shape_four = (components, slots_here, cells_edge, cells_edge)
    y_low = jnp.tile(ghost_faces[:, :, 2].reshape(shape_four), (1, 1, 1, cells_edge))
    y_high = jnp.tile(ghost_faces[:, :, 3].reshape(shape_four), (1, 1, 1, cells_edge))
    z_low = jnp.repeat(ghost_faces[:, :, 4].reshape(shape_four), cells_edge, axis=3)
    z_high = jnp.repeat(ghost_faces[:, :, 5].reshape(shape_four), cells_edge, axis=3)
    zero_row = jnp.zeros_like(volume[..., :cells_edge])
    zero_cell = jnp.zeros_like(volume[..., :1])
    y_minus = jnp.where(lane_y == 0, y_low, jnp.concatenate([zero_row, volume[..., :-cells_edge]], axis=-1))
    y_plus = jnp.where(lane_y == cells_edge - 1, y_high, jnp.concatenate([volume[..., cells_edge:], zero_row], axis=-1))
    z_minus = jnp.where(lane_z == 0, z_low, jnp.concatenate([zero_cell, volume[..., :-1]], axis=-1))
    z_plus = jnp.where(lane_z == cells_edge - 1, z_high, jnp.concatenate([volume[..., 1:], zero_cell], axis=-1))
    neighbor_sum = x_minus + x_plus + y_minus + y_plus + z_minus + z_plus - 6.0 * volume
    return volume + step_rate * visc_cells[None] * neighbor_sum


def reference(coarse_field, fine_field, viscosity, corners, grid_slot, neighbors):
    slot_total = fine_field.shape[1]
    grid_total = corners.shape[0]
    grid_ids = jnp.arange(grid_total, dtype=jnp.int32)
    slot_ids = jnp.arange(slot_total, dtype=jnp.int32)
    slot_match = grid_slot[None, :] == slot_ids[:, None]
    slot_active = jnp.any(slot_match, axis=1)
    slot_grid = jnp.sum(jnp.where(slot_match, grid_ids[None, :], 0), axis=1).astype(jnp.int32)
    box_corner = corners[slot_grid].astype(jnp.int32)
    padded = jnp.pad(coarse_field, ((0, 0), (1, 1), (1, 1), (1, 1)))
    zero_start = jnp.zeros((), jnp.int32)

    def cut_cube(corner):
        return lax.dynamic_slice(padded, (zero_start, corner[0], corner[1], corner[2]), (3, B + 2, B + 2, B + 2))

    cubes = jax.vmap(cut_cube)(box_corner)
    tangent, low_side, high_side = tables()
    highest = lax.Precision.HIGHEST
    face_list = [
        jnp.einsum('nkabc,a,sb,tc->knst', cubes, low_side, tangent, tangent, precision=highest),
        jnp.einsum('nkabc,a,sb,tc->knst', cubes, high_side, tangent, tangent, precision=highest),
        jnp.einsum('nkabc,sa,b,tc->knst', cubes, tangent, low_side, tangent, precision=highest),
        jnp.einsum('nkabc,sa,b,tc->knst', cubes, tangent, high_side, tangent, precision=highest),
        jnp.einsum('nkabc,sa,tb,c->knst', cubes, tangent, tangent, low_side, precision=highest),
        jnp.einsum('nkabc,sa,tb,c->knst', cubes, tangent, tangent, high_side, precision=highest),
    ]
    ghost_faces = jnp.stack([face.reshape(3, slot_total, F * F) for face in face_list], axis=2)
    near_grid = neighbors[slot_grid]
    near_slot = grid_slot[jnp.maximum(near_grid, 0)]
    from_low = fine_field[:, near_slot[:, 0], F - 1, :]
    from_high = fine_field[:, near_slot[:, 1], 0, :]
    has_near = (near_grid >= 0) & slot_active[:, None]
    lower_plane = jnp.where(has_near[None, :, 0, None], from_low, ghost_faces[:, :, 0])
    upper_plane = jnp.where(has_near[None, :, 1, None], from_high, ghost_faces[:, :, 1])
    advanced = advance(fine_field, viscosity, ghost_faces, lower_plane, upper_plane)
    fine_out = jnp.where(slot_active[None, :, None, None], advanced, 0.0)
    averages = advanced.reshape(3, slot_total, B, 2, B, 2, B, 2).mean(axis=(3, 5, 7))

    def place_box(index, field_now):
        corner = box_corner[index]
        start = (zero_start, corner[0], corner[1], corner[2])
        current = lax.dynamic_slice(field_now, start, (3, B, B, B))
        value = jnp.where(slot_active[index], averages[:, index], current)
        return lax.dynamic_update_slice(field_now, value, start)

    coarse_out = lax.fori_loop(0, slot_total, place_box, coarse_field)
    return fine_out, coarse_out
```

```python
import functools
import numpy as np
import jax
import jax.numpy as jnp
from jax import lax
from jax.experimental import pallas as pl
from jax.experimental.pallas import tpu as pltpu
from jax.sharding import PartitionSpec as P

B = 8
F = 16
SLOTS = 4
SIDE = B + 2
LANES = 128
MEAN_ROWS = 16
step_rate = 0.15
HIGHEST = lax.Precision.HIGHEST


def up(n, m):
    return -(-n // m) * m


def tables():
    tangent = np.zeros((F, SIDE), np.float32)
    for f in range(F):
        c = f // 2 + 1
        tangent[f, c] = 0.75
        tangent[f, c - 1 if f % 2 == 0 else c + 1] = 0.25
    low = np.zeros((SIDE,), np.float32)
    low[0], low[1] = 0.75, 0.25
    return tangent, low, low[::-1].copy()


def ghost_matrix():
    tangent, low, high = tables()
    out = np.zeros((LANES, 2 * F * F), np.float32)
    edge = np.zeros((SIDE, SIDE, F, F), np.float32)
    edge[:, :, 0, :] += np.einsum("b,tc->bct", low, tangent)
    edge[:, :, F - 1, :] += np.einsum("b,tc->bct", high, tangent)
    edge[:, :, :, 0] += np.einsum("sb,c->bcs", tangent, low)
    edge[:, :, :, F - 1] += np.einsum("sb,c->bcs", tangent, high)
    out[: SIDE * SIDE, : F * F] = edge.reshape(SIDE * SIDE, F * F)
    out[: SIDE * SIDE, F * F :] = np.einsum("sb,tc->bcst", tangent, tangent).reshape(SIDE * SIDE, F * F)
    return out


def mean_matrices():
    lanes = np.zeros((F * F, LANES), np.float32)
    for y in range(F):
        for z in range(F):
            for half in range(2):
                lanes[y * F + z, half * 64 + (y // 2) * B + z // 2] = 0.125
    rows = np.zeros((2, SLOTS * MEAN_ROWS, 3 * SLOTS * F), np.float32)
    for half in range(2):
        for s in range(SLOTS):
            for k in range(3):
                for a in range(B // 2):
                    for p in range(2):
                        x = 2 * (half * (B // 2) + a) + p
                        rows[half, s * MEAN_ROWS + k * (B // 2) + a, (k * SLOTS + s) * F + x] = 1.0
    return lanes, rows


def dot(a, b):
    return jnp.dot(a, b, precision=HIGHEST, preferred_element_type=jnp.float32)


def fine_kernel(
    nx, ny, flags, slab, planes, fine, visc, kw, tmat, nmat, lane_mean, row_mean,
    fine_out, picked, slabs, plane_buf, mean_send, means, advs, send_sem, recv_sem, own_sem,
):
    count = nx * ny
    me = lax.axis_index("gx") * ny + lax.axis_index("gy")

    def peer(o):
        t = lax.rem(me + o, count)
        return {"gx": t // ny, "gy": lax.rem(t, ny)}

    def remote(o, which, src, dst):
        return pltpu.make_async_remote_copy(
            src_ref=src, dst_ref=dst, send_sem=send_sem.at[which, o], recv_sem=recv_sem.at[which, o],
            device_id=peer(o), device_id_type=pl.DeviceIdType.MESH,
        )

    def slab_copy(o):
        return remote(o, 0, slab, slabs.at[me])

    def plane_copy(o):
        return remote(o, 1, planes, plane_buf.at[pl.ds(me * SLOTS, SLOTS)])

    def mean_copy(o):
        return remote(o, 2, mean_send, means.at[pl.ds(me * SLOTS, SLOTS)])

    barrier = pltpu.get_barrier_semaphore()

    def greet(o, c):
        pl.semaphore_signal(barrier, inc=1, device_id=peer(o), device_id_type=pl.DeviceIdType.MESH)
        return c

    lax.fori_loop(1, count, greet, 0)
    own_slab = pltpu.make_async_copy(slab, slabs.at[me], own_sem.at[0])
    own_plane = pltpu.make_async_copy(planes, plane_buf.at[pl.ds(me * SLOTS, SLOTS)], own_sem.at[1])
    own_slab.start()
    own_plane.start()
    pl.semaphore_wait(barrier, count - 1)

    def send(o, c):
        slab_copy(o).start()
        plane_copy(o).start()
        return c

    lax.fori_loop(1, count, send, 0)
    own_slab.wait()
    own_plane.wait()

    def finish(o, c):
        slab_copy(o).wait()
        plane_copy(o).wait()
        return c

    lax.fori_loop(1, count, finish, 0)

    half = dot(slabs[flags[0]], kw[...])
    ghost = dot(tmat[...], half[:, : F * F])
    xface = dot(nmat[...], half[:, F * F :])
    lane = lax.broadcasted_iota(jnp.int32, (F, F * F), 1)
    row = lax.broadcasted_iota(jnp.int32, (F, F * F), 0)
    lz = lane % F
    for s in range(SLOTS):
        active = flags[1 + s] > 0
        low_near = plane_buf[flags[1 + SLOTS + s]]
        high_near = plane_buf[flags[1 + 2 * SLOTS + s]]
        has_low = flags[1 + 3 * SLOTS + s] > 0
        has_high = flags[1 + 4 * SLOTS + s] > 0
        for k in range(3):
            v = fine[k, s]
            r = (k * SLOTS + s) * 2
            lower = jnp.where(has_low, low_near[2 * k : 2 * k + 1], xface[r : r + 1])
            upper = jnp.where(has_high, high_near[2 * k + 1 : 2 * k + 2], xface[r + 1 : r + 2])
            total = jnp.where(row == 0, lower, pltpu.roll(v, 1, 0))
            total += jnp.where(row == F - 1, upper, pltpu.roll(v, F - 1, 0))
            total += jnp.where(lane < F, 0.0, pltpu.roll(v, F, 1))
            total += jnp.where(lane >= F * F - F, 0.0, pltpu.roll(v, F * F - F, 1))
            total += jnp.where(lz == 0, 0.0, pltpu.roll(v, 1, 1))
            total += jnp.where(lz == F - 1, 0.0, pltpu.roll(v, F * F - 1, 1))
            at = (k * SLOTS + s) * F
            total += ghost[at : at + F] - 6.0 * v
            adv = v + step_rate * visc[s] * total
            advs[at : at + F] = adv
            fine_out[k, s] = jnp.where(active, adv, 0.0)
    z = dot(advs[...], lane_mean[...])
    first = dot(row_mean[0], z)
    second = dot(row_mean[1], z)
    lane_m = lax.broadcasted_iota(jnp.int32, first.shape, 1)
    packed = jnp.where(lane_m < 64, first, second).reshape(SLOTS, MEAN_ROWS, LANES)
    mean_send[...] = packed
    for s in range(SLOTS):
        means[me * SLOTS + s] = packed[s]

    def send_mean(o, c):
        mean_copy(o).start()
        return c

    lax.fori_loop(1, count, send_mean, 0)

    def finish_mean(o, c):
        mean_copy(o).wait()
        return c

    lax.fori_loop(1, count, finish_mean, 0)
    for s in range(SLOTS):
        picked[s] = means[flags[1 + 5 * SLOTS + s]]


def coarse_kernel(at, field, rows, out):
    n = field.shape[0]
    out[...] = field[...]
    y = pl.multiple_of(at[0], B)
    z = at[1]
    r3 = lax.broadcast_in_dim(rows[...], (n, B, B * B), (0, 2))
    sub = lax.broadcasted_iota(jnp.int32, r3.shape, 1)
    ln = lax.broadcasted_iota(jnp.int32, r3.shape, 2)
    spread = jnp.where(ln // B == sub, r3, 0.0).reshape(n * B, B * B)
    width = field.shape[2]
    c_id = lax.broadcasted_iota(jnp.int32, (B * B, width), 0) % B
    z_id = lax.broadcasted_iota(jnp.int32, (B * B, width), 1)
    place = jnp.where(z_id == z + c_id, 1.0, 0.0)
    value = dot(spread, place).reshape(n, B, width)
    z3 = lax.broadcasted_iota(jnp.int32, value.shape, 2)
    inside = (z3 >= z) & (z3 < z + B) & (at[2] > 0)
    out[:, pl.ds(y, B), :] = jnp.where(inside, value, field[:, pl.ds(y, B), :])


def shift(low_part, high_part, axis):
    count = lax.axis_size(axis)
    low = lax.ppermute(high_part, axis, [(i, i + 1) for i in range(count - 1)])
    high = lax.ppermute(low_part, axis, [(i + 1, i) for i in range(count - 1)])
    return low, high


def cut_slab(field, y, z):
    nx, ny, nz = field.shape[1:]
    zlo, zhi = shift(field[..., :1], field[..., -1:], "gz")

    def wide(part, lo, hi):
        return jnp.concatenate([lo, part, hi], axis=3)

    first = wide(field[:, :1], zlo[:, :1], zhi[:, :1])
    last = wide(field[:, -1:], zlo[:, -1:], zhi[:, -1:])
    xlo, xhi = shift(first, last, "gx")

    def line(start, size):
        def cut(a):
            return lax.dynamic_slice_in_dim(a, start, size, axis=2)

        return jnp.concatenate([cut(xlo), wide(cut(field), cut(zlo), cut(zhi)), cut(xhi)], axis=1)

    ylo, yhi = shift(line(0, 1), line(ny - 1, 1), "gy")

    def zcut(a):
        return lax.dynamic_slice_in_dim(a, z, SIDE, axis=3)

    low = jnp.where(y == 0, zcut(ylo), zcut(line(jnp.maximum(y - 1, 0), 1)))
    high = jnp.where(y == ny - B, zcut(yhi), zcut(line(jnp.minimum(y + B, ny - 1), 1)))
    slab = jnp.concatenate([low, zcut(line(y, B)), high], axis=2)
    slab = slab.reshape(3 * (nx + 2), SIDE * SIDE)
    rows = up(3 * (nx + 2), 8)
    return jnp.pad(slab, ((0, rows - 3 * (nx + 2)), (0, LANES - SIDE * SIDE)))


def on_device(coarse_field, fine_field, viscosity, corners, grid_slot, neighbors):
    count_x = lax.axis_size("gx")
    count_y = lax.axis_size("gy")
    count_z = lax.axis_size("gz")
    count = count_x * count_y
    index_x = lax.axis_index("gx")
    index_y = lax.axis_index("gy")
    index_z = lax.axis_index("gz")
    brick_x, brick_y, brick_z = coarse_field.shape[1:]
    my_device = (index_x * count_y + index_y) * count_z + index_z
    slot_range = jnp.arange(SLOTS, dtype=jnp.int32)
    home_x = corners[:, 0] // brick_x
    home_y = corners[:, 1] // brick_y
    home_z = corners[:, 2] // brick_z
    in_brick = (home_x == index_x) & (home_y == index_y) & (home_z == index_z)
    box_x = (corners[:, 0] - home_x * brick_x) // B
    owner_row = grid_slot // (SLOTS * count_z) * SLOTS + grid_slot % SLOTS

    def pick(match, values):
        return jnp.sum(jnp.where(match, values[None, :], 0), axis=1)

    present = jnp.any(in_brick)
    anchor_y = jnp.max(jnp.where(in_brick, corners[:, 1] - index_y * brick_y, 0))
    anchor_z = jnp.max(jnp.where(in_brick, corners[:, 2] - index_z * brick_z, 0))
    row_match = in_brick[None, :] & (box_x[None, :] == slot_range[:, None])
    need_mean = pick(row_match, owner_row)
    own_match = grid_slot[None, :] == (my_device * SLOTS + slot_range)[:, None]
    active = jnp.any(own_match, axis=1)
    slot_box = pick(own_match, box_x)
    home = jnp.max(jnp.where(own_match, (home_x * count_y + home_y)[None, :], 0))
    near_low = pick(own_match, neighbors[:, 0])
    near_high = pick(own_match, neighbors[:, 1])
    has_low = active & (near_low >= 0)
    has_high = active & (near_high >= 0)
    grid_ids = jnp.arange(corners.shape[0], dtype=jnp.int32)
    low_row = pick(grid_ids[None, :] == near_low[:, None], owner_row)
    high_row = pick(grid_ids[None, :] == near_high[:, None], owner_row)
    flags = jnp.concatenate(
        [home[None], active.astype(jnp.int32), low_row, high_row,
         has_low.astype(jnp.int32), has_high.astype(jnp.int32), need_mean]
    ).astype(jnp.int32)

    slab = cut_slab(coarse_field, anchor_y, anchor_z)
    slab_rows = slab.shape[0]
    planes = jnp.stack([fine_field[:, :, F - 1, :], fine_field[:, :, 0, :]], axis=1)
    planes = planes.reshape(6, SLOTS, F * F).transpose(1, 0, 2)
    planes = jnp.pad(planes, ((0, 0), (0, 2), (0, 0)))

    k_id = jnp.arange(3, dtype=jnp.int32)[:, None, None, None]
    i_id = jnp.arange(F, dtype=jnp.int32)[None, None, :, None]
    r_id = jnp.arange(slab_rows, dtype=jnp.int32)[None, None, None, :]
    base = k_id * (brick_x + 2) + B * slot_box[None, :, None, None]
    center = i_id // 2 + 1
    other = jnp.where(i_id % 2 == 0, center - 1, center + 1)
    tmat = jnp.where(r_id == base + center, 0.75, jnp.where(r_id == base + other, 0.25, 0.0))
    tmat = tmat.reshape(3 * SLOTS * F, slab_rows).astype(jnp.float32)
    side_id = jnp.arange(2, dtype=jnp.int32)[None, None, :, None]
    outer = jnp.where(side_id == 0, 0, SIDE - 1)
    inner = jnp.where(side_id == 0, 1, SIDE - 2)
    nmat = jnp.where(r_id == base + outer, 0.75, jnp.where(r_id == base + inner, 0.25, 0.0))
    nmat = nmat.reshape(3 * SLOTS * 2, slab_rows).astype(jnp.float32)

    lane_mean, row_mean = mean_matrices()
    vmem = pl.BlockSpec(memory_space=pltpu.VMEM)
    fine_out, picked = pl.pallas_call(
        functools.partial(fine_kernel, count_x, count_y),
        out_shape=(
            jax.ShapeDtypeStruct(fine_field.shape, jnp.float32),
            jax.ShapeDtypeStruct((SLOTS, MEAN_ROWS, LANES), jnp.float32),
        ),
        in_specs=[pl.BlockSpec(memory_space=pltpu.SMEM)] + [vmem] * 9,
        out_specs=(vmem, vmem),
        scratch_shapes=[
            pltpu.VMEM((count, slab_rows, LANES), jnp.float32),
            pltpu.VMEM((count * SLOTS, 8, F * F), jnp.float32),
            pltpu.VMEM((SLOTS, MEAN_ROWS, LANES), jnp.float32),
            pltpu.VMEM((count * SLOTS, MEAN_ROWS, LANES), jnp.float32),
            pltpu.VMEM((3 * SLOTS * F, F * F), jnp.float32),
            pltpu.SemaphoreType.DMA((3, count)),
            pltpu.SemaphoreType.DMA((3, count)),
            pltpu.SemaphoreType.DMA((2,)),
        ],
        compiler_params=pltpu.CompilerParams(collective_id=0, has_side_effects=True),
        name="fine_step",
    )(
        flags, slab, planes, fine_field, viscosity, jnp.asarray(ghost_matrix()), tmat, nmat,
        jnp.asarray(lane_mean), jnp.asarray(row_mean),
    )
    rows = picked[:, : 3 * (B // 2)].reshape(SLOTS, 3, B // 2, 2, B * B)
    rows = rows.transpose(1, 0, 3, 2, 4).reshape(3 * brick_x, B * B)
    at = jnp.stack([anchor_y, anchor_z, present.astype(jnp.int32)]).astype(jnp.int32)
    block = 16
    coarse_out = pl.pallas_call(
        coarse_kernel,
        out_shape=jax.ShapeDtypeStruct((3 * brick_x, brick_y, brick_z), jnp.float32),
        grid_spec=pltpu.PrefetchScalarGridSpec(
            num_scalar_prefetch=1,
            grid=(3 * brick_x // block,),
            in_specs=[
                pl.BlockSpec((block, brick_y, brick_z), lambda i, at: (i, 0, 0)),
                pl.BlockSpec((block, B * B), lambda i, at: (i, 0)),
            ],
            out_specs=pl.BlockSpec((block, brick_y, brick_z), lambda i, at: (i, 0, 0)),
        ),
        name="coarse_fill",
    )(at, coarse_field.reshape(3 * brick_x, brick_y, brick_z), rows)
    return fine_out, coarse_out.reshape(coarse_field.shape)


def solution(mesh):
    in_specs = (
        P(None, "gx", "gy", "gz"),
        P(None, ("gx", "gy", "gz"), None, None),
        P(("gx", "gy", "gz"), None, None),
        P(),
        P(),
        P(),
    )
    out_specs = (P(None, ("gx", "gy", "gz"), None, None), P(None, "gx", "gy", "gz"))
    return jax.shard_map(
        on_device, mesh=mesh, in_specs=in_specs, out_specs=out_specs, check_vma=False
    )
```

```python
import functools
import numpy as np
import jax
import jax.numpy as jnp
from jax import lax
from jax.experimental import pallas as pl
from jax.experimental.pallas import tpu as pltpu
from jax.sharding import PartitionSpec as P

B = 8
F = 16
SLOTS = 4
SIDE = B + 2
LANES = 128
MEAN_ROWS = 12
PLANES = 4
PLANE_ROWS = 6
step_rate = 0.15
HIGHEST = lax.Precision.HIGHEST


def up(n, m):
    return -(-n // m) * m


def tables():
    tangent = np.zeros((F, SIDE), np.float32)
    for f in range(F):
        c = f // 2 + 1
        tangent[f, c] = 0.75
        tangent[f, c - 1 if f % 2 == 0 else c + 1] = 0.25
    low = np.zeros((SIDE,), np.float32)
    low[0], low[1] = 0.75, 0.25
    return tangent, low, low[::-1].copy()


def edge_matrices(nx):
    tangent, low, high = tables()
    eye = np.eye(SIDE, dtype=np.float32)
    wide = 4 * SIDE
    cut = np.zeros((SIDE, SIDE, 4, SIDE), np.float32)
    cut[:, :, 0] = np.einsum("b,cd->bcd", low, eye)
    cut[:, :, 1] = np.einsum("b,cd->bcd", high, eye)
    cut[:, :, 2] = np.einsum("bd,c->bcd", eye, low)
    cut[:, :, 3] = np.einsum("bd,c->bcd", eye, high)
    put = np.zeros((4, SIDE, F, F), np.float32)
    put[0, :, 0, :] = tangent.T
    put[1, :, F - 1, :] = tangent.T
    put[2, :, :, 0] = tangent.T
    put[3, :, :, F - 1] = tangent.T
    rows = up(3 * nx, 8)
    edge_rows = up(nx + 6, 8)
    columns = np.zeros((3, LANES, LANES), np.float32)
    places = np.zeros((3, LANES, F * F), np.float32)
    lines = np.zeros((4, edge_rows, rows), np.float32)
    for k in range(3):
        columns[k, : SIDE * SIDE, k * wide : (k + 1) * wide] = cut.reshape(SIDE * SIDE, wide)
        places[k, k * wide : (k + 1) * wide] = put.reshape(wide, F * F)
        lines[k, np.arange(nx), k * nx + np.arange(nx)] = 1.0
        for row, outer, inner in ((0, 0, 1), (1, nx - 1, nx - 2)):
            lines[3, nx + 2 * k + row, k * nx + outer] = 0.75
            lines[3, nx + 2 * k + row, k * nx + inner] = 0.25
    across = np.zeros((LANES, F * F), np.float32)
    across[: SIDE * SIDE] = np.einsum("sb,tc->bcst", tangent, tangent).reshape(SIDE * SIDE, F * F)
    return columns, lines, places, across


def mean_matrices():
    lanes = np.zeros((F * F, LANES), np.float32)
    for y in range(F):
        for z in range(F):
            for half in range(2):
                lanes[y * F + z, half * 64 + (y // 2) * B + z // 2] = 0.125
    rows = np.zeros((2, SLOTS * MEAN_ROWS, 3 * SLOTS * F), np.float32)
    for half in range(2):
        for s in range(SLOTS):
            for k in range(3):
                for a in range(B // 2):
                    for p in range(2):
                        x = 2 * (half * (B // 2) + a) + p
                        rows[half, s * MEAN_ROWS + k * (B // 2) + a, (k * SLOTS + s) * F + x] = 1.0
    return lanes, rows


def dot(a, b):
    return jnp.dot(a, b, precision=HIGHEST, preferred_element_type=jnp.float32)


def edge_kernel(chosen, slab, fine, columns, lines, edges, planes):
    total = dot(lines[3], slab[...])
    for k in range(3):
        total += dot(lines[k], dot(slab[...], columns[k]))
    edges[...] = total
    for p in range(PLANES):
        slot = chosen[p] // 2
        low_side = chosen[p] % 2 == 0
        for k in range(3):
            v = fine[k, slot]
            line = jnp.where(low_side, v[F - 1 : F], v[0:1])
            for h in range(2):
                at = p * PLANE_ROWS + k * 2 + h
                planes[at : at + 1] = line[:, h * LANES : (h + 1) * LANES]


def fine_kernel(
    nx, ny, width, flags, edges, planes, fine, visc, places, across, lane_mean, row_mean,
    fine_out, picked, slabs, plane_buf, mean_send, means, advs, send_sem, recv_sem, own_sem,
):
    count = nx * ny
    me = lax.axis_index("gx") * ny + lax.axis_index("gy")

    def peer(o):
        t = lax.rem(me + o, count)
        return {"gx": t // ny, "gy": lax.rem(t, ny)}

    def remote(o, which, src, dst):
        return pltpu.make_async_remote_copy(
            src_ref=src, dst_ref=dst, send_sem=send_sem.at[which, o], recv_sem=recv_sem.at[which, o],
            device_id=peer(o), device_id_type=pl.DeviceIdType.MESH,
        )

    def slab_copy(o):
        return remote(o, 0, edges, slabs.at[me])

    def plane_copy(o):
        return remote(o, 1, planes, plane_buf.at[me])

    def mean_copy(o):
        return remote(o, 2, mean_send, means.at[me])

    barrier = pltpu.get_barrier_semaphore()

    def greet(o, c):
        pl.semaphore_signal(barrier, inc=1, device_id=peer(o), device_id_type=pl.DeviceIdType.MESH)
        return c

    lax.fori_loop(1, count, greet, 0)
    own_slab = pltpu.make_async_copy(edges, slabs.at[me], own_sem.at[0])
    own_plane = pltpu.make_async_copy(planes, plane_buf.at[me], own_sem.at[1])
    own_slab.start()
    own_plane.start()
    pl.semaphore_wait(barrier, count - 1)

    def send(o, c):
        slab_copy(o).start()
        plane_copy(o).start()
        return c

    lax.fori_loop(1, count, send, 0)
    own_slab.wait()
    own_plane.wait()

    def finish(o, c):
        slab_copy(o).wait()
        plane_copy(o).wait()
        return c

    lax.fori_loop(1, count, finish, 0)

    def flag(group, s):
        return flags[1 + group * SLOTS + s]

    mine = slabs[flags[0]]
    shape = (SLOTS * F, mine.shape[0])
    line_id = lax.broadcasted_iota(jnp.int32, shape, 0)
    from_row = lax.broadcasted_iota(jnp.int32, shape, 1)
    box = jnp.full(shape, flag(1, 0), jnp.int32)
    for s in range(1, SLOTS):
        box = jnp.where(line_id // F == s, flag(1, s), box)
    i_id = line_id % F
    center = B * box + i_id // 2 + 1
    other = jnp.where(i_id % 2 == 0, center - 1, center + 1)
    blend = jnp.where(from_row == center, 0.75, jnp.where(from_row == other, 0.25, 0.0))
    along = dot(blend, mine)
    ghosts = [dot(along, places[k]) for k in range(3)]
    xface = dot(mine, across[...])[width : width + 6]
    lane = lax.broadcasted_iota(jnp.int32, (F, F * F), 1)
    row = lax.broadcasted_iota(jnp.int32, (F, F * F), 0)
    lz = lane % F
    for s in range(SLOTS):
        active = flag(0, s) > 0
        near = []
        for side in range(2):
            base = 2 + 5 * side
            far = plane_buf[flag(base, s)]
            rank = flag(base + 1, s)
            chosen = far[:PLANE_ROWS]
            for p in range(1, PLANES):
                chosen = jnp.where(rank == p, far[p * PLANE_ROWS : (p + 1) * PLANE_ROWS], chosen)
            near.append((chosen, flag(base + 2, s), flag(base + 3, s) > 0, flag(base + 4, s) > 0))
        for k in range(3):
            v = fine[k, s]
            ends = []
            for side in range(2):
                chosen, slot, local, has = near[side]
                x = (F - 1) * (1 - side)
                far = jnp.concatenate([chosen[2 * k : 2 * k + 1], chosen[2 * k + 1 : 2 * k + 2]], axis=1)
                here = fine[k, slot][x : x + 1]
                outer = xface[2 * k + side : 2 * k + side + 1]
                ends.append(jnp.where(has, jnp.where(local, here, far), outer))
            lower, upper = ends
            total = jnp.where(row == 0, lower, pltpu.roll(v, 1, 0))
            total += jnp.where(row == F - 1, upper, pltpu.roll(v, F - 1, 0))
            total += jnp.where(lane < F, 0.0, pltpu.roll(v, F, 1))
            total += jnp.where(lane >= F * F - F, 0.0, pltpu.roll(v, F * F - F, 1))
            total += jnp.where(lz == 0, 0.0, pltpu.roll(v, 1, 1))
            total += jnp.where(lz == F - 1, 0.0, pltpu.roll(v, F * F - 1, 1))
            at = (k * SLOTS + s) * F
            total += ghosts[k][s * F : s * F + F] - 6.0 * v
            adv = v + step_rate * visc[s] * total
            advs[at : at + F] = adv
            fine_out[k, s] = jnp.where(active, adv, 0.0)
    z = dot(advs[...], lane_mean[...])
    first = dot(row_mean[0], z)
    second = dot(row_mean[1], z)
    lane_m = lax.broadcasted_iota(jnp.int32, first.shape, 1)
    packed = jnp.where(lane_m < 64, first, second)
    mean_send[...] = packed
    means[me] = packed

    def send_mean(o, c):
        mean_copy(o).start()
        return c

    lax.fori_loop(1, count, send_mean, 0)

    def finish_mean(o, c):
        mean_copy(o).wait()
        return c

    lax.fori_loop(1, count, finish_mean, 0)
    for s in range(SLOTS):
        got = means[flag(12, s)]
        part = flag(13, s)
        value = got[:MEAN_ROWS]
        for p in range(1, SLOTS):
            value = jnp.where(part == p, got[p * MEAN_ROWS : (p + 1) * MEAN_ROWS], value)
        picked[s] = value


def coarse_kernel(at, field, rows, out):
    n = field.shape[0]
    out[...] = field[...]
    y = pl.multiple_of(at[0], B)
    z = at[1]
    r3 = lax.broadcast_in_dim(rows[...], (n, B, B * B), (0, 2))
    sub = lax.broadcasted_iota(jnp.int32, r3.shape, 1)
    ln = lax.broadcasted_iota(jnp.int32, r3.shape, 2)
    spread = jnp.where(ln // B == sub, r3, 0.0).reshape(n * B, B * B)
    width = field.shape[2]
    c_id = lax.broadcasted_iota(jnp.int32, (B * B, width), 0) % B
    z_id = lax.broadcasted_iota(jnp.int32, (B * B, width), 1)
    place = jnp.where(z_id == z + c_id, 1.0, 0.0)
    value = dot(spread, place).reshape(n, B, width)
    z3 = lax.broadcasted_iota(jnp.int32, value.shape, 2)
    inside = (z3 >= z) & (z3 < z + B) & (at[2] > 0)
    out[:, pl.ds(y, B), :] = jnp.where(inside, value, field[:, pl.ds(y, B), :])


def shift(low_part, high_part, axis):
    count = lax.axis_size(axis)
    low = lax.ppermute(high_part, axis, [(i, i + 1) for i in range(count - 1)])
    high = lax.ppermute(low_part, axis, [(i + 1, i) for i in range(count - 1)])
    return low, high


def cut_slab(field, y, z):
    nx, ny, nz = field.shape[1:]
    zlo, zhi = shift(field[..., :1], field[..., -1:], "gz")

    def wide(part, lo, hi):
        return jnp.concatenate([lo, part, hi], axis=3)

    first = wide(field[:, :1], zlo[:, :1], zhi[:, :1])
    last = wide(field[:, -1:], zlo[:, -1:], zhi[:, -1:])
    xlo, xhi = shift(first, last, "gx")

    def line(start, size):
        def cut(a):
            return lax.dynamic_slice_in_dim(a, start, size, axis=2)

        return jnp.concatenate([cut(xlo), wide(cut(field), cut(zlo), cut(zhi)), cut(xhi)], axis=1)

    ylo, yhi = shift(line(0, 1), line(ny - 1, 1), "gy")

    def zcut(a):
        return lax.dynamic_slice_in_dim(a, z, SIDE, axis=3)

    low = jnp.where(y == 0, zcut(ylo), zcut(line(jnp.maximum(y - 1, 0), 1)))
    high = jnp.where(y == ny - B, zcut(yhi), zcut(line(jnp.minimum(y + B, ny - 1), 1)))
    slab = jnp.concatenate([low, zcut(line(y, B)), high], axis=2)
    slab = slab.reshape(3 * (nx + 2), SIDE * SIDE)
    rows = up(3 * (nx + 2), 8)
    return jnp.pad(slab, ((0, rows - 3 * (nx + 2)), (0, LANES - SIDE * SIDE)))


def on_device(coarse_field, fine_field, viscosity, corners, grid_slot, neighbors):
    count_x = lax.axis_size("gx")
    count_y = lax.axis_size("gy")
    count_z = lax.axis_size("gz")
    count = count_x * count_y
    index_x = lax.axis_index("gx")
    index_y = lax.axis_index("gy")
    index_z = lax.axis_index("gz")
    brick_x, brick_y, brick_z = coarse_field.shape[1:]
    my_device = (index_x * count_y + index_y) * count_z + index_z
    slot_range = jnp.arange(SLOTS, dtype=jnp.int32)
    home_x = corners[:, 0] // brick_x
    home_y = corners[:, 1] // brick_y
    home_z = corners[:, 2] // brick_z
    in_brick = (home_x == index_x) & (home_y == index_y) & (home_z == index_z)
    box_x = (corners[:, 0] - home_x * brick_x) // B
    owner_group = grid_slot // (SLOTS * count_z)
    owner_slot = grid_slot % SLOTS
    owner_dev = grid_slot // SLOTS
    grid_ids = jnp.arange(corners.shape[0], dtype=jnp.int32)

    def pick(match, values):
        return jnp.sum(jnp.where(match, values[None, :], 0), axis=1)

    present = jnp.any(in_brick)
    anchor_y = jnp.max(jnp.where(in_brick, corners[:, 1] - index_y * brick_y, 0))
    anchor_z = jnp.max(jnp.where(in_brick, corners[:, 2] - index_z * brick_z, 0))
    row_match = in_brick[None, :] & (box_x[None, :] == slot_range[:, None])
    need_mean = pick(row_match, grid_slot)
    own_match = grid_slot[None, :] == (my_device * SLOTS + slot_range)[:, None]
    active = jnp.any(own_match, axis=1)
    slot_box = pick(own_match, box_x)
    home = jnp.max(jnp.where(own_match, (home_x * count_y + home_y)[None, :], 0))
    near_low = pick(own_match, neighbors[:, 0])
    near_high = pick(own_match, neighbors[:, 1])

    leaves = []
    for side in range(2):
        near_all = neighbors[:, 1 - side]
        near_dev = pick(grid_ids[None, :] == near_all[:, None], owner_dev)
        leaves.append((near_all >= 0) & (near_dev != owner_dev))
    same = owner_dev[None, :] == owner_dev[:, None]
    ahead = same & (owner_slot[None, :] < owner_slot[:, None])
    before = pick(ahead, leaves[0].astype(jnp.int32) + leaves[1].astype(jnp.int32))
    ranks = (before, before + leaves[0].astype(jnp.int32))
    own = owner_dev == my_device
    plane_range = jnp.arange(PLANES, dtype=jnp.int32)
    chosen = jnp.zeros((PLANES,), jnp.int32)
    for side in range(2):
        match = (own & leaves[side])[None, :] & (ranks[side][None, :] == plane_range[:, None])
        chosen = chosen + pick(match, owner_slot * 2 + side)
    parts = [home[None], active.astype(jnp.int32), slot_box]
    for side, near in ((0, near_low), (1, near_high)):
        match = grid_ids[None, :] == near[:, None]
        local = pick(match, owner_dev) == my_device
        parts += [
            pick(match, owner_group),
            pick(match, ranks[side]),
            pick(match, owner_slot),
            local.astype(jnp.int32),
            (active & (near >= 0)).astype(jnp.int32),
        ]
    parts += [need_mean // (SLOTS * count_z), need_mean % SLOTS]
    flags = jnp.concatenate(parts).astype(jnp.int32)

    slab = cut_slab(coarse_field, anchor_y, anchor_z)
    columns, lines, places, across = edge_matrices(brick_x + 2)
    edge_rows = lines.shape[1]
    vmem = pl.BlockSpec(memory_space=pltpu.VMEM)
    smem = pl.BlockSpec(memory_space=pltpu.SMEM)
    edges, planes = pl.pallas_call(
        edge_kernel,
        out_shape=(
            jax.ShapeDtypeStruct((edge_rows, LANES), jnp.float32),
            jax.ShapeDtypeStruct((PLANES * PLANE_ROWS, LANES), jnp.float32),
        ),
        in_specs=[smem] + [vmem] * 4,
        out_specs=(vmem, vmem),
        name="edge_cut",
    )(chosen, slab, fine_field, jnp.asarray(columns), jnp.asarray(lines))

    lane_mean, row_mean = mean_matrices()
    fine_out, picked = pl.pallas_call(
        functools.partial(fine_kernel, count_x, count_y, brick_x + 2),
        out_shape=(
            jax.ShapeDtypeStruct(fine_field.shape, jnp.float32),
            jax.ShapeDtypeStruct((SLOTS, MEAN_ROWS, LANES), jnp.float32),
        ),
        in_specs=[smem] + [vmem] * 8,
        out_specs=(vmem, vmem),
        scratch_shapes=[
            pltpu.VMEM((count, edge_rows, LANES), jnp.float32),
            pltpu.VMEM((count, PLANES * PLANE_ROWS, LANES), jnp.float32),
            pltpu.VMEM((SLOTS * MEAN_ROWS, LANES), jnp.float32),
            pltpu.VMEM((count, SLOTS * MEAN_ROWS, LANES), jnp.float32),
            pltpu.VMEM((3 * SLOTS * F, F * F), jnp.float32),
            pltpu.SemaphoreType.DMA((3, count)),
            pltpu.SemaphoreType.DMA((3, count)),
            pltpu.SemaphoreType.DMA((2,)),
        ],
        compiler_params=pltpu.CompilerParams(collective_id=0, has_side_effects=True),
        name="fine_step",
    )(
        flags, edges, planes, fine_field, viscosity, jnp.asarray(places), jnp.asarray(across),
        jnp.asarray(lane_mean), jnp.asarray(row_mean),
    )
    rows = picked[:, : 3 * (B // 2)].reshape(SLOTS, 3, B // 2, 2, B * B)
    rows = rows.transpose(1, 0, 3, 2, 4).reshape(3 * brick_x, B * B)
    at = jnp.stack([anchor_y, anchor_z, present.astype(jnp.int32)]).astype(jnp.int32)
    block = 16
    coarse_out = pl.pallas_call(
        coarse_kernel,
        out_shape=jax.ShapeDtypeStruct((3 * brick_x, brick_y, brick_z), jnp.float32),
        grid_spec=pltpu.PrefetchScalarGridSpec(
            num_scalar_prefetch=1,
            grid=(3 * brick_x // block,),
            in_specs=[
                pl.BlockSpec((block, brick_y, brick_z), lambda i, at: (i, 0, 0)),
                pl.BlockSpec((block, B * B), lambda i, at: (i, 0)),
            ],
            out_specs=pl.BlockSpec((block, brick_y, brick_z), lambda i, at: (i, 0, 0)),
        ),
        name="coarse_fill",
    )(at, coarse_field.reshape(3 * brick_x, brick_y, brick_z), rows)
    return fine_out, coarse_out.reshape(coarse_field.shape)


def solution(mesh):
    in_specs = (
        P(None, "gx", "gy", "gz"),
        P(None, ("gx", "gy", "gz"), None, None),
        P(("gx", "gy", "gz"), None, None),
        P(),
        P(),
        P(),
    )
    out_specs = (P(None, ("gx", "gy", "gz"), None, None), P(None, "gx", "gy", "gz"))
    return jax.shard_map(
        on_device, mesh=mesh, in_specs=in_specs, out_specs=out_specs, check_vma=False
    )
```

```python
import functools
import numpy as np
import jax
import jax.numpy as jnp
from jax import lax
from jax.experimental import pallas as pl
from jax.experimental.pallas import tpu as pltpu
from jax.sharding import PartitionSpec as P

B = 8
F = 16
SLOTS = 4
SIDE = B + 2
LANES = 128
MEAN_ROWS = 12
PLANES = 4
PLANE_ROWS = 6
step_rate = 0.15
HIGHEST = lax.Precision.HIGHEST


def up(n, m):
    return -(-n // m) * m


def tables():
    tangent = np.zeros((F, SIDE), np.float32)
    for f in range(F):
        c = f // 2 + 1
        tangent[f, c] = 0.75
        tangent[f, c - 1 if f % 2 == 0 else c + 1] = 0.25
    low = np.zeros((SIDE,), np.float32)
    low[0], low[1] = 0.75, 0.25
    return tangent, low, low[::-1].copy()


def edge_matrices(nx):
    tangent, low, high = tables()
    eye = np.eye(SIDE, dtype=np.float32)
    wide = 4 * SIDE
    cut = np.zeros((SIDE, SIDE, 4, SIDE), np.float32)
    cut[:, :, 0] = np.einsum("b,cd->bcd", low, eye)
    cut[:, :, 1] = np.einsum("b,cd->bcd", high, eye)
    cut[:, :, 2] = np.einsum("bd,c->bcd", eye, low)
    cut[:, :, 3] = np.einsum("bd,c->bcd", eye, high)
    put = np.zeros((4, SIDE, F, F), np.float32)
    put[0, :, 0, :] = tangent.T
    put[1, :, F - 1, :] = tangent.T
    put[2, :, :, 0] = tangent.T
    put[3, :, :, F - 1] = tangent.T
    rows = up(3 * nx, 8)
    edge_rows = up(nx + 6, 8)
    columns = np.zeros((3, LANES, LANES), np.float32)
    places = np.zeros((3, LANES, F * F), np.float32)
    lines = np.zeros((4, edge_rows, rows), np.float32)
    for k in range(3):
        columns[k, : SIDE * SIDE, k * wide : (k + 1) * wide] = cut.reshape(SIDE * SIDE, wide)
        places[k, k * wide : (k + 1) * wide] = put.reshape(wide, F * F)
        lines[k, np.arange(nx), k * nx + np.arange(nx)] = 1.0
        for row, outer, inner in ((0, 0, 1), (1, nx - 1, nx - 2)):
            lines[3, nx + 2 * k + row, k * nx + outer] = 0.75
            lines[3, nx + 2 * k + row, k * nx + inner] = 0.25
    across = np.zeros((LANES, F * F), np.float32)
    across[: SIDE * SIDE] = np.einsum("sb,tc->bcst", tangent, tangent).reshape(SIDE * SIDE, F * F)
    return columns, lines, places, across


def mean_matrices():
    lanes = np.zeros((F * F, LANES), np.float32)
    for y in range(F):
        for z in range(F):
            for half in range(2):
                lanes[y * F + z, half * 64 + (y // 2) * B + z // 2] = 0.125
    rows = np.zeros((2, SLOTS * MEAN_ROWS, 3 * SLOTS * F), np.float32)
    for half in range(2):
        for s in range(SLOTS):
            for k in range(3):
                for a in range(B // 2):
                    for p in range(2):
                        x = 2 * (half * (B // 2) + a) + p
                        rows[half, s * MEAN_ROWS + k * (B // 2) + a, (k * SLOTS + s) * F + x] = 1.0
    return lanes, rows


def dot(a, b):
    return jnp.dot(a, b, precision=HIGHEST, preferred_element_type=jnp.float32)


def edge_kernel(chosen, slab, fine, columns, lines, edges, planes):
    total = dot(lines[3], slab[...])
    for k in range(3):
        total += dot(lines[k], dot(slab[...], columns[k]))
    edges[...] = total
    for p in range(PLANES):
        slot = chosen[p] // 2
        low_side = chosen[p] % 2 == 0
        for k in range(3):
            v = fine[k, slot]
            line = jnp.where(low_side, v[F - 1 : F], v[0:1])
            for h in range(2):
                at = p * PLANE_ROWS + k * 2 + h
                planes[at : at + 1] = line[:, h * LANES : (h + 1) * LANES]


def fine_kernel(
    nx, ny, width, flags, edges, planes, fine, visc, places, across, lane_mean, row_mean,
    fine_out, picked, slabs, plane_buf, mean_send, means, advs, send_sem, recv_sem, own_sem,
):
    count = nx * ny
    me = lax.axis_index("gx") * ny + lax.axis_index("gy")

    def peer(o):
        t = lax.rem(me + o, count)
        return {"gx": t // ny, "gy": lax.rem(t, ny)}

    def remote(o, which, src, dst):
        return pltpu.make_async_remote_copy(
            src_ref=src, dst_ref=dst, send_sem=send_sem.at[which, o], recv_sem=recv_sem.at[which, o],
            device_id=peer(o), device_id_type=pl.DeviceIdType.MESH,
        )

    def slab_copy(o):
        return remote(o, 0, edges, slabs.at[me])

    def plane_copy(o):
        return remote(o, 1, planes, plane_buf.at[me])

    def mean_copy(o):
        return remote(o, 2, mean_send, means.at[me])

    barrier = pltpu.get_barrier_semaphore()

    def greet(o, c):
        pl.semaphore_signal(barrier, inc=1, device_id=peer(o), device_id_type=pl.DeviceIdType.MESH)
        return c

    lax.fori_loop(1, count, greet, 0)
    own_slab = pltpu.make_async_copy(edges, slabs.at[me], own_sem.at[0])
    own_plane = pltpu.make_async_copy(planes, plane_buf.at[me], own_sem.at[1])
    own_slab.start()
    own_plane.start()
    pl.semaphore_wait(barrier, count - 1)

    def send(o, c):
        slab_copy(o).start()
        plane_copy(o).start()
        return c

    lax.fori_loop(1, count, send, 0)
    own_slab.wait()
    own_plane.wait()

    def finish(o, c):
        slab_copy(o).wait()
        plane_copy(o).wait()
        return c

    lax.fori_loop(1, count, finish, 0)

    def flag(group, s):
        return flags[1 + group * SLOTS + s]

    mine = slabs[flags[0]]
    shape = (SLOTS * F, mine.shape[0])
    line_id = lax.broadcasted_iota(jnp.int32, shape, 0)
    from_row = lax.broadcasted_iota(jnp.int32, shape, 1)
    box = jnp.full(shape, flag(1, 0), jnp.int32)
    for s in range(1, SLOTS):
        box = jnp.where(line_id // F == s, flag(1, s), box)
    i_id = line_id % F
    center = B * box + i_id // 2 + 1
    other = jnp.where(i_id % 2 == 0, center - 1, center + 1)
    blend = jnp.where(from_row == center, 0.75, jnp.where(from_row == other, 0.25, 0.0))
    along = dot(blend, mine)
    ghosts = [dot(along, places[k]) for k in range(3)]
    xface = dot(mine, across[...])[width : width + 6]
    lane = lax.broadcasted_iota(jnp.int32, (F, F * F), 1)
    row = lax.broadcasted_iota(jnp.int32, (F, F * F), 0)
    lz = lane % F
    for s in range(SLOTS):
        active = flag(0, s) > 0
        near = []
        for side in range(2):
            base = 2 + 5 * side
            far = plane_buf[flag(base, s)]
            rank = flag(base + 1, s)
            chosen = far[:PLANE_ROWS]
            for p in range(1, PLANES):
                chosen = jnp.where(rank == p, far[p * PLANE_ROWS : (p + 1) * PLANE_ROWS], chosen)
            near.append((chosen, flag(base + 2, s), flag(base + 3, s) > 0, flag(base + 4, s) > 0))
        for k in range(3):
            v = fine[k, s]
            ends = []
            for side in range(2):
                chosen, slot, local, has = near[side]
                x = (F - 1) * (1 - side)
                far = jnp.concatenate([chosen[2 * k : 2 * k + 1], chosen[2 * k + 1 : 2 * k + 2]], axis=1)
                here = fine[k, slot][x : x + 1]
                outer = xface[2 * k + side : 2 * k + side + 1]
                ends.append(jnp.where(has, jnp.where(local, here, far), outer))
            lower, upper = ends
            total = jnp.where(row == 0, lower, pltpu.roll(v, 1, 0))
            total += jnp.where(row == F - 1, upper, pltpu.roll(v, F - 1, 0))
            total += jnp.where(lane < F, 0.0, pltpu.roll(v, F, 1))
            total += jnp.where(lane >= F * F - F, 0.0, pltpu.roll(v, F * F - F, 1))
            total += jnp.where(lz == 0, 0.0, pltpu.roll(v, 1, 1))
            total += jnp.where(lz == F - 1, 0.0, pltpu.roll(v, F * F - 1, 1))
            at = (k * SLOTS + s) * F
            total += ghosts[k][s * F : s * F + F] - 6.0 * v
            adv = v + step_rate * visc[s] * total
            advs[at : at + F] = adv
            fine_out[k, s] = jnp.where(active, adv, 0.0)
    z = dot(advs[...], lane_mean[...])
    first = dot(row_mean[0], z)
    second = dot(row_mean[1], z)
    lane_m = lax.broadcasted_iota(jnp.int32, first.shape, 1)
    packed = jnp.where(lane_m < 64, first, second)
    mean_send[...] = packed
    means[me] = packed

    def send_mean(o, c):
        mean_copy(o).start()
        return c

    lax.fori_loop(1, count, send_mean, 0)

    def finish_mean(o, c):
        mean_copy(o).wait()
        return c

    lax.fori_loop(1, count, finish_mean, 0)
    for s in range(SLOTS):
        got = means[flag(12, s)]
        part = flag(13, s)
        value = got[:MEAN_ROWS]
        for p in range(1, SLOTS):
            value = jnp.where(part == p, got[p * MEAN_ROWS : (p + 1) * MEAN_ROWS], value)
        picked[s] = value


def plan_kernel(ny, nz, bricks, corners, grid_slot, neighbors, flags, at, chosen, held):
    ix, iy, iz = lax.axis_index("gx"), lax.axis_index("gy"), lax.axis_index("gz")
    device = (ix * ny + iy) * nz + iz
    total = held.shape[0]

    def put(group, s, value):
        flags[1 + group * SLOTS + s] = value

    def clear(i, c):
        for j in range(8):
            held[i * 8 + j] = -1
        return c

    lax.fori_loop(0, total // 8, clear, 0)
    for s in range(SLOTS):
        put(12, s, 0)
        put(13, s, 0)
        chosen[s] = 0
    for i in range(3):
        at[i] = 0

    def scan(g, c):
        held[grid_slot[g]] = g
        x, y, z = corners[0, g], corners[1, g], corners[2, g]
        mine = (x // bricks[0] == ix) & (y // bricks[1] == iy) & (z // bricks[2] == iz)

        @pl.when(mine)
        def _():
            box = lax.rem(x, bricks[0]) // B
            flags[1 + 12 * SLOTS + box] = grid_slot[g] // (SLOTS * nz)
            flags[1 + 13 * SLOTS + box] = lax.rem(grid_slot[g], SLOTS)
            at[0] = lax.rem(y, bricks[1])
            at[1] = lax.rem(z, bricks[2])
            at[2] = 1

        return c

    lax.fori_loop(0, grid_slot.shape[0], scan, 0)

    def leaves(n, side):
        grid = held[n]
        near = neighbors[1 - side, jnp.maximum(grid, 0)]
        other = grid_slot[jnp.maximum(near, 0)] // SLOTS
        return jnp.where((grid >= 0) & (near >= 0) & (other != n // SLOTS), 1, 0)

    def rank_of(n, side):
        first = n // SLOTS * SLOTS
        rank = 0 if side == 0 else leaves(n, 0)
        for s in range(SLOTS):
            both = leaves(first + s, 0) + leaves(first + s, 1)
            rank = rank + jnp.where(first + s < n, both, 0)
        return rank

    home = jnp.int32(0)
    count = jnp.int32(0)
    for s in range(SLOTS):
        n = device * SLOTS + s
        grid = held[n]
        active = grid >= 0
        g = jnp.maximum(grid, 0)
        put(0, s, jnp.where(active, 1, 0))
        put(1, s, jnp.where(active, lax.rem(corners[0, g], bricks[0]) // B, 0))
        here = corners[0, g] // bricks[0] * ny + corners[1, g] // bricks[1]
        home = jnp.where(active, here, home)
        for side in range(2):
            base = 2 + 5 * side
            near = neighbors[side, g]
            m = grid_slot[jnp.maximum(near, 0)]
            put(base, s, m // (SLOTS * nz))
            put(base + 1, s, rank_of(m, side))
            put(base + 2, s, lax.rem(m, SLOTS))
            put(base + 3, s, jnp.where(m // SLOTS == device, 1, 0))
            put(base + 4, s, jnp.where(active & (near >= 0), 1, 0))
        for side in range(2):
            out = leaves(n, side)

            @pl.when(out > 0)
            def _():
                chosen[count] = s * 2 + side

            count = count + out
    flags[0] = home


def coarse_kernel(at, field, rows, out):
    n = field.shape[0]
    out[...] = field[...]
    y = pl.multiple_of(at[0], B)
    z = at[1]
    r3 = lax.broadcast_in_dim(rows[...], (n, B, B * B), (0, 2))
    sub = lax.broadcasted_iota(jnp.int32, r3.shape, 1)
    ln = lax.broadcasted_iota(jnp.int32, r3.shape, 2)
    spread = jnp.where(ln // B == sub, r3, 0.0).reshape(n * B, B * B)
    width = field.shape[2]
    c_id = lax.broadcasted_iota(jnp.int32, (B * B, width), 0) % B
    z_id = lax.broadcasted_iota(jnp.int32, (B * B, width), 1)
    place = jnp.where(z_id == z + c_id, 1.0, 0.0)
    value = dot(spread, place).reshape(n, B, width)
    z3 = lax.broadcasted_iota(jnp.int32, value.shape, 2)
    inside = (z3 >= z) & (z3 < z + B) & (at[2] > 0)
    out[:, pl.ds(y, B), :] = jnp.where(inside, value, field[:, pl.ds(y, B), :])


def shift(low_part, high_part, axis):
    count = lax.axis_size(axis)
    low = lax.ppermute(high_part, axis, [(i, i + 1) for i in range(count - 1)])
    high = lax.ppermute(low_part, axis, [(i + 1, i) for i in range(count - 1)])
    return low, high


def cut_slab(field, y, z):
    nx, ny, nz = field.shape[1:]
    if lax.axis_size("gz") == 2:
        upper = lax.axis_index("gz") == 1
        other = lax.ppermute(jnp.where(upper, field[..., :1], field[..., -1:]), "gz", [(0, 1), (1, 0)])
        zlo, zhi = jnp.where(upper, other, 0.0), jnp.where(upper, 0.0, other)
    else:
        zlo, zhi = shift(field[..., :1], field[..., -1:], "gz")

    def wide(part, lo, hi):
        return jnp.concatenate([lo, part, hi], axis=3)

    first = wide(field[:, :1], zlo[:, :1], zhi[:, :1])
    last = wide(field[:, -1:], zlo[:, -1:], zhi[:, -1:])
    xlo, xhi = shift(first, last, "gx")

    def line(start, size):
        def cut(a):
            return lax.dynamic_slice_in_dim(a, start, size, axis=2)

        return jnp.concatenate([cut(xlo), wide(cut(field), cut(zlo), cut(zhi)), cut(xhi)], axis=1)

    ylo, yhi = shift(line(0, 1), line(ny - 1, 1), "gy")

    def zcut(a):
        return lax.dynamic_slice_in_dim(a, z, SIDE, axis=3)

    low = jnp.where(y == 0, zcut(ylo), zcut(line(jnp.maximum(y - 1, 0), 1)))
    high = jnp.where(y == ny - B, zcut(yhi), zcut(line(jnp.minimum(y + B, ny - 1), 1)))
    slab = jnp.concatenate([low, zcut(line(y, B)), high], axis=2)
    slab = slab.reshape(3 * (nx + 2), SIDE * SIDE)
    rows = up(3 * (nx + 2), 8)
    return jnp.pad(slab, ((0, rows - 3 * (nx + 2)), (0, LANES - SIDE * SIDE)))


def on_device(coarse_field, fine_field, viscosity, corners, grid_slot, neighbors):
    count_x = lax.axis_size("gx")
    count_y = lax.axis_size("gy")
    count_z = lax.axis_size("gz")
    count = count_x * count_y
    brick_x, brick_y, brick_z = coarse_field.shape[1:]
    smem = pl.BlockSpec(memory_space=pltpu.SMEM)
    flags, at, chosen = pl.pallas_call(
        functools.partial(plan_kernel, count_y, count_z, (brick_x, brick_y, brick_z)),
        out_shape=(
            jax.ShapeDtypeStruct((1 + 14 * SLOTS,), jnp.int32),
            jax.ShapeDtypeStruct((3,), jnp.int32),
            jax.ShapeDtypeStruct((PLANES,), jnp.int32),
        ),
        in_specs=[smem] * 3,
        out_specs=(smem, smem, smem),
        scratch_shapes=[pltpu.SMEM((count * count_z * SLOTS,), jnp.int32)],
        name="plan",
    )(corners.T, grid_slot, neighbors.T)
    anchor_y, anchor_z = at[0], at[1]

    slab = cut_slab(coarse_field, anchor_y, anchor_z)
    columns, lines, places, across = edge_matrices(brick_x + 2)
    edge_rows = lines.shape[1]
    vmem = pl.BlockSpec(memory_space=pltpu.VMEM)
    edges, planes = pl.pallas_call(
        edge_kernel,
        out_shape=(
            jax.ShapeDtypeStruct((edge_rows, LANES), jnp.float32),
            jax.ShapeDtypeStruct((PLANES * PLANE_ROWS, LANES), jnp.float32),
        ),
        in_specs=[smem] + [vmem] * 4,
        out_specs=(vmem, vmem),
        name="edge_cut",
    )(chosen, slab, fine_field, jnp.asarray(columns), jnp.asarray(lines))

    lane_mean, row_mean = mean_matrices()
    fine_out, picked = pl.pallas_call(
        functools.partial(fine_kernel, count_x, count_y, brick_x + 2),
        out_shape=(
            jax.ShapeDtypeStruct(fine_field.shape, jnp.float32),
            jax.ShapeDtypeStruct((SLOTS, MEAN_ROWS, LANES), jnp.float32),
        ),
        in_specs=[smem] + [vmem] * 8,
        out_specs=(vmem, vmem),
        scratch_shapes=[
            pltpu.VMEM((count, edge_rows, LANES), jnp.float32),
            pltpu.VMEM((count, PLANES * PLANE_ROWS, LANES), jnp.float32),
            pltpu.VMEM((SLOTS * MEAN_ROWS, LANES), jnp.float32),
            pltpu.VMEM((count, SLOTS * MEAN_ROWS, LANES), jnp.float32),
            pltpu.VMEM((3 * SLOTS * F, F * F), jnp.float32),
            pltpu.SemaphoreType.DMA((3, count)),
            pltpu.SemaphoreType.DMA((3, count)),
            pltpu.SemaphoreType.DMA((2,)),
        ],
        compiler_params=pltpu.CompilerParams(collective_id=0, has_side_effects=True),
        name="fine_step",
    )(
        flags, edges, planes, fine_field, viscosity, jnp.asarray(places), jnp.asarray(across),
        jnp.asarray(lane_mean), jnp.asarray(row_mean),
    )
    rows = picked[:, : 3 * (B // 2)].reshape(SLOTS, 3, B // 2, 2, B * B)
    rows = rows.transpose(1, 0, 3, 2, 4).reshape(3 * brick_x, B * B)
    block = 16
    coarse_out = pl.pallas_call(
        coarse_kernel,
        out_shape=jax.ShapeDtypeStruct((3 * brick_x, brick_y, brick_z), jnp.float32),
        grid_spec=pltpu.PrefetchScalarGridSpec(
            num_scalar_prefetch=1,
            grid=(3 * brick_x // block,),
            in_specs=[
                pl.BlockSpec((block, brick_y, brick_z), lambda i, at: (i, 0, 0)),
                pl.BlockSpec((block, B * B), lambda i, at: (i, 0)),
            ],
            out_specs=pl.BlockSpec((block, brick_y, brick_z), lambda i, at: (i, 0, 0)),
        ),
        name="coarse_fill",
    )(at, coarse_field.reshape(3 * brick_x, brick_y, brick_z), rows)
    return fine_out, coarse_out.reshape(coarse_field.shape)


def solution(mesh):
    in_specs = (
        P(None, "gx", "gy", "gz"),
        P(None, ("gx", "gy", "gz"), None, None),
        P(("gx", "gy", "gz"), None, None),
        P(),
        P(),
        P(),
    )
    out_specs = (P(None, ("gx", "gy", "gz"), None, None), P(None, "gx", "gy", "gz"))
    return jax.shard_map(
        on_device, mesh=mesh, in_specs=in_specs, out_specs=out_specs, check_vma=False
    )
```

```python
import functools
import numpy as np
import jax
import jax.numpy as jnp
from jax import lax
from jax.experimental import pallas as pl
from jax.experimental.pallas import tpu as pltpu
from jax.sharding import PartitionSpec as P

B = 8
F = 16
SLOTS = 4
SIDE = B + 2
LANES = 128
MEAN_ROWS = 12
PLANES = 4
PLANE_ROWS = 6
step_rate = 0.15
HIGHEST = lax.Precision.HIGHEST


def up(n, m):
    return -(-n // m) * m


def tables():
    tangent = np.zeros((F, SIDE), np.float32)
    for f in range(F):
        c = f // 2 + 1
        tangent[f, c] = 0.75
        tangent[f, c - 1 if f % 2 == 0 else c + 1] = 0.25
    low = np.zeros((SIDE,), np.float32)
    low[0], low[1] = 0.75, 0.25
    return tangent, low, low[::-1].copy()


def edge_matrices(nx):
    tangent, low, high = tables()
    eye = np.eye(SIDE, dtype=np.float32)
    wide = 4 * SIDE
    cut = np.zeros((SIDE, SIDE, 4, SIDE), np.float32)
    cut[:, :, 0] = np.einsum("b,cd->bcd", low, eye)
    cut[:, :, 1] = np.einsum("b,cd->bcd", high, eye)
    cut[:, :, 2] = np.einsum("bd,c->bcd", eye, low)
    cut[:, :, 3] = np.einsum("bd,c->bcd", eye, high)
    put = np.zeros((4, SIDE, F, F), np.float32)
    put[0, :, 0, :] = tangent.T
    put[1, :, F - 1, :] = tangent.T
    put[2, :, :, 0] = tangent.T
    put[3, :, :, F - 1] = tangent.T
    rows = up(3 * nx, 8)
    edge_rows = up(nx + 6, 8)
    columns = np.zeros((3, LANES, LANES), np.float32)
    places = np.zeros((3, LANES, F * F), np.float32)
    lines = np.zeros((4, edge_rows, rows), np.float32)
    for k in range(3):
        columns[k, : SIDE * SIDE, k * wide : (k + 1) * wide] = cut.reshape(SIDE * SIDE, wide)
        places[k, k * wide : (k + 1) * wide] = put.reshape(wide, F * F)
        lines[k, np.arange(nx), k * nx + np.arange(nx)] = 1.0
        for row, outer, inner in ((0, 0, 1), (1, nx - 1, nx - 2)):
            lines[3, nx + 2 * k + row, k * nx + outer] = 0.75
            lines[3, nx + 2 * k + row, k * nx + inner] = 0.25
    across = np.zeros((LANES, F * F), np.float32)
    across[: SIDE * SIDE] = np.einsum("sb,tc->bcst", tangent, tangent).reshape(SIDE * SIDE, F * F)
    return columns, lines, places, across


def mean_matrices():
    lanes = np.zeros((F * F, LANES), np.float32)
    for y in range(F):
        for z in range(F):
            for half in range(2):
                lanes[y * F + z, half * 64 + (y // 2) * B + z // 2] = 0.125
    rows = np.zeros((2, SLOTS * MEAN_ROWS, 3 * SLOTS * F), np.float32)
    for half in range(2):
        for s in range(SLOTS):
            for k in range(3):
                for a in range(B // 2):
                    for p in range(2):
                        x = 2 * (half * (B // 2) + a) + p
                        rows[half, s * MEAN_ROWS + k * (B // 2) + a, (k * SLOTS + s) * F + x] = 1.0
    return lanes, rows


def dot(a, b):
    return jnp.dot(a, b, precision=HIGHEST, preferred_element_type=jnp.float32)


def edge_kernel(chosen, slab, fine, columns, lines, edges, planes):
    total = dot(lines[3], slab[...])
    for k in range(3):
        total += dot(lines[k], dot(slab[...], columns[k]))
    edges[...] = total
    for p in range(PLANES):
        slot = chosen[p] // 2
        low_side = chosen[p] % 2 == 0
        for k in range(3):
            v = fine[k, slot]
            line = jnp.where(low_side, v[F - 1 : F], v[0:1])
            for h in range(2):
                at = p * PLANE_ROWS + k * 2 + h
                planes[at : at + 1] = line[:, h * LANES : (h + 1) * LANES]


def fine_kernel(
    nx, ny, width, flags, edges, planes, fine, visc, places, across, lane_mean, row_mean,
    fine_out, picked, slabs, plane_buf, mean_send, means, advs, send_sem, recv_sem, own_sem,
):
    count = nx * ny
    me = lax.axis_index("gx") * ny + lax.axis_index("gy")

    def peer(o):
        t = lax.rem(me + o, count)
        return {"gx": t // ny, "gy": lax.rem(t, ny)}

    def remote(o, which, src, dst):
        return pltpu.make_async_remote_copy(
            src_ref=src, dst_ref=dst, send_sem=send_sem.at[which, o], recv_sem=recv_sem.at[which, o],
            device_id=peer(o), device_id_type=pl.DeviceIdType.MESH,
        )

    def slab_copy(o):
        return remote(o, 0, edges, slabs.at[me])

    def plane_copy(o):
        return remote(o, 1, planes, plane_buf.at[me])

    def mean_copy(o):
        return remote(o, 2, mean_send, means.at[me])

    barrier = pltpu.get_barrier_semaphore()

    def greet(o, c):
        pl.semaphore_signal(barrier, inc=1, device_id=peer(o), device_id_type=pl.DeviceIdType.MESH)
        return c

    lax.fori_loop(1, count, greet, 0)
    own_slab = pltpu.make_async_copy(edges, slabs.at[me], own_sem.at[0])
    own_plane = pltpu.make_async_copy(planes, plane_buf.at[me], own_sem.at[1])
    own_slab.start()
    own_plane.start()
    pl.semaphore_wait(barrier, count - 1)

    def send_slab(o, c):
        slab_copy(o).start()
        return c

    def send_plane(o, c):
        plane_copy(o).start()
        return c

    lax.fori_loop(1, count, send_slab, 0)
    lax.fori_loop(1, count, send_plane, 0)
    own_slab.wait()
    own_plane.wait()

    def finish_slab(o, c):
        slab_copy(o).wait()
        return c

    def finish_plane(o, c):
        plane_copy(o).wait()
        return c

    lax.fori_loop(1, count, finish_slab, 0)

    def flag(group, s):
        return flags[1 + group * SLOTS + s]

    mine = slabs[flags[0]]
    shape = (SLOTS * F, mine.shape[0])
    line_id = lax.broadcasted_iota(jnp.int32, shape, 0)
    from_row = lax.broadcasted_iota(jnp.int32, shape, 1)
    box = jnp.full(shape, flag(1, 0), jnp.int32)
    for s in range(1, SLOTS):
        box = jnp.where(line_id // F == s, flag(1, s), box)
    i_id = line_id % F
    center = B * box + i_id // 2 + 1
    other = jnp.where(i_id % 2 == 0, center - 1, center + 1)
    blend = jnp.where(from_row == center, 0.75, jnp.where(from_row == other, 0.25, 0.0))
    along = dot(blend, mine)
    ghosts = [dot(along, places[k]) for k in range(3)]
    xface = dot(mine, across[...])[width : width + 6]
    lax.fori_loop(1, count, finish_plane, 0)
    lane = lax.broadcasted_iota(jnp.int32, (F, F * F), 1)
    row = lax.broadcasted_iota(jnp.int32, (F, F * F), 0)
    lz = lane % F
    for s in range(SLOTS):
        active = flag(0, s) > 0
        near = []
        for side in range(2):
            base = 2 + 5 * side
            far = plane_buf[flag(base, s)]
            rank = flag(base + 1, s)
            chosen = far[:PLANE_ROWS]
            for p in range(1, PLANES):
                chosen = jnp.where(rank == p, far[p * PLANE_ROWS : (p + 1) * PLANE_ROWS], chosen)
            near.append((chosen, flag(base + 2, s), flag(base + 3, s) > 0, flag(base + 4, s) > 0))
        for k in range(3):
            v = fine[k, s]
            ends = []
            for side in range(2):
                chosen, slot, local, has = near[side]
                x = (F - 1) * (1 - side)
                far = jnp.concatenate([chosen[2 * k : 2 * k + 1], chosen[2 * k + 1 : 2 * k + 2]], axis=1)
                here = fine[k, slot][x : x + 1]
                outer = xface[2 * k + side : 2 * k + side + 1]
                ends.append(jnp.where(has, jnp.where(local, here, far), outer))
            lower, upper = ends
            total = jnp.where(row == 0, lower, pltpu.roll(v, 1, 0))
            total += jnp.where(row == F - 1, upper, pltpu.roll(v, F - 1, 0))
            total += jnp.where(lane < F, 0.0, pltpu.roll(v, F, 1))
            total += jnp.where(lane >= F * F - F, 0.0, pltpu.roll(v, F * F - F, 1))
            total += jnp.where(lz == 0, 0.0, pltpu.roll(v, 1, 1))
            total += jnp.where(lz == F - 1, 0.0, pltpu.roll(v, F * F - 1, 1))
            at = (k * SLOTS + s) * F
            total += ghosts[k][s * F : s * F + F] - 6.0 * v
            adv = v + step_rate * visc[s] * total
            advs[at : at + F] = adv
            fine_out[k, s] = jnp.where(active, adv, 0.0)
    z = dot(advs[...], lane_mean[...])
    first = dot(row_mean[0], z)
    second = dot(row_mean[1], z)
    lane_m = lax.broadcasted_iota(jnp.int32, first.shape, 1)
    packed = jnp.where(lane_m < 64, first, second)
    mean_send[...] = packed
    means[me] = packed

    def send_mean(o, c):
        mean_copy(o).start()
        return c

    lax.fori_loop(1, count, send_mean, 0)

    def finish_mean(o, c):
        mean_copy(o).wait()
        return c

    lax.fori_loop(1, count, finish_mean, 0)
    for s in range(SLOTS):
        got = means[flag(12, s)]
        part = flag(13, s)
        value = got[:MEAN_ROWS]
        for p in range(1, SLOTS):
            value = jnp.where(part == p, got[p * MEAN_ROWS : (p + 1) * MEAN_ROWS], value)
        picked[s] = value


def plan_kernel(ny, nz, bricks, corners, grid_slot, neighbors, flags, at, chosen, held):
    ix, iy, iz = lax.axis_index("gx"), lax.axis_index("gy"), lax.axis_index("gz")
    device = (ix * ny + iy) * nz + iz
    total = held.shape[0]

    def put(group, s, value):
        flags[1 + group * SLOTS + s] = value

    def clear(i, c):
        for j in range(8):
            held[i * 8 + j] = -1
        return c

    lax.fori_loop(0, total // 8, clear, 0)
    for s in range(SLOTS):
        put(12, s, 0)
        put(13, s, 0)
        chosen[s] = 0
    for i in range(3):
        at[i] = 0

    def scan(g, c):
        held[grid_slot[g]] = g
        x, y, z = corners[0, g], corners[1, g], corners[2, g]
        mine = (x // bricks[0] == ix) & (y // bricks[1] == iy) & (z // bricks[2] == iz)

        @pl.when(mine)
        def _():
            box = lax.rem(x, bricks[0]) // B
            flags[1 + 12 * SLOTS + box] = grid_slot[g] // (SLOTS * nz)
            flags[1 + 13 * SLOTS + box] = lax.rem(grid_slot[g], SLOTS)
            at[0] = lax.rem(y, bricks[1])
            at[1] = lax.rem(z, bricks[2])
            at[2] = 1

        return c

    lax.fori_loop(0, grid_slot.shape[0], scan, 0)

    def leaves(n, side):
        grid = held[n]
        near = neighbors[1 - side, jnp.maximum(grid, 0)]
        other = grid_slot[jnp.maximum(near, 0)] // SLOTS
        return jnp.where((grid >= 0) & (near >= 0) & (other != n // SLOTS), 1, 0)

    def rank_of(n, side):
        first = n // SLOTS * SLOTS
        rank = 0 if side == 0 else leaves(n, 0)
        for s in range(SLOTS):
            both = leaves(first + s, 0) + leaves(first + s, 1)
            rank = rank + jnp.where(first + s < n, both, 0)
        return rank

    home = jnp.int32(0)
    count = jnp.int32(0)
    for s in range(SLOTS):
        n = device * SLOTS + s
        grid = held[n]
        active = grid >= 0
        g = jnp.maximum(grid, 0)
        put(0, s, jnp.where(active, 1, 0))
        put(1, s, jnp.where(active, lax.rem(corners[0, g], bricks[0]) // B, 0))
        here = corners[0, g] // bricks[0] * ny + corners[1, g] // bricks[1]
        home = jnp.where(active, here, home)
        for side in range(2):
            base = 2 + 5 * side
            near = neighbors[side, g]
            m = grid_slot[jnp.maximum(near, 0)]
            put(base, s, m // (SLOTS * nz))
            put(base + 1, s, rank_of(m, side))
            put(base + 2, s, lax.rem(m, SLOTS))
            put(base + 3, s, jnp.where(m // SLOTS == device, 1, 0))
            put(base + 4, s, jnp.where(active & (near >= 0), 1, 0))
        for side in range(2):
            out = leaves(n, side)

            @pl.when(out > 0)
            def _():
                chosen[count] = s * 2 + side

            count = count + out
    flags[0] = home


def coarse_kernel(at, field, rows, out):
    n = field.shape[0]
    out[...] = field[...]
    y = pl.multiple_of(at[0], B)
    z = at[1]
    r3 = lax.broadcast_in_dim(rows[...], (n, B, B * B), (0, 2))
    sub = lax.broadcasted_iota(jnp.int32, r3.shape, 1)
    ln = lax.broadcasted_iota(jnp.int32, r3.shape, 2)
    spread = jnp.where(ln // B == sub, r3, 0.0).reshape(n * B, B * B)
    width = field.shape[2]
    c_id = lax.broadcasted_iota(jnp.int32, (B * B, width), 0) % B
    z_id = lax.broadcasted_iota(jnp.int32, (B * B, width), 1)
    place = jnp.where(z_id == z + c_id, 1.0, 0.0)
    value = dot(spread, place).reshape(n, B, width)
    z3 = lax.broadcasted_iota(jnp.int32, value.shape, 2)
    inside = (z3 >= z) & (z3 < z + B) & (at[2] > 0)
    out[:, pl.ds(y, B), :] = jnp.where(inside, value, field[:, pl.ds(y, B), :])


def shift(low_part, high_part, axis):
    count = lax.axis_size(axis)
    low = lax.ppermute(high_part, axis, [(i, i + 1) for i in range(count - 1)])
    high = lax.ppermute(low_part, axis, [(i + 1, i) for i in range(count - 1)])
    return low, high


def cut_slab(field, y, z):
    nx, ny, nz = field.shape[1:]
    if lax.axis_size("gz") == 2:
        upper = lax.axis_index("gz") == 1
        other = lax.ppermute(jnp.where(upper, field[..., :1], field[..., -1:]), "gz", [(0, 1), (1, 0)])
        zlo, zhi = jnp.where(upper, other, 0.0), jnp.where(upper, 0.0, other)
    else:
        zlo, zhi = shift(field[..., :1], field[..., -1:], "gz")

    def wide(part, lo, hi):
        return jnp.concatenate([lo, part, hi], axis=3)

    first = wide(field[:, :1], zlo[:, :1], zhi[:, :1])
    last = wide(field[:, -1:], zlo[:, -1:], zhi[:, -1:])
    xlo, xhi = shift(first, last, "gx")

    def line(start, size):
        def cut(a):
            return lax.dynamic_slice_in_dim(a, start, size, axis=2)

        return jnp.concatenate([cut(xlo), wide(cut(field), cut(zlo), cut(zhi)), cut(xhi)], axis=1)

    ylo, yhi = shift(line(0, 1), line(ny - 1, 1), "gy")

    def zcut(a):
        return lax.dynamic_slice_in_dim(a, z, SIDE, axis=3)

    low = jnp.where(y == 0, zcut(ylo), zcut(line(jnp.maximum(y - 1, 0), 1)))
    high = jnp.where(y == ny - B, zcut(yhi), zcut(line(jnp.minimum(y + B, ny - 1), 1)))
    slab = jnp.concatenate([low, zcut(line(y, B)), high], axis=2)
    slab = slab.reshape(3 * (nx + 2), SIDE * SIDE)
    rows = up(3 * (nx + 2), 8)
    return jnp.pad(slab, ((0, rows - 3 * (nx + 2)), (0, LANES - SIDE * SIDE)))


def on_device(coarse_field, fine_field, viscosity, corners, grid_slot, neighbors):
    count_x = lax.axis_size("gx")
    count_y = lax.axis_size("gy")
    count_z = lax.axis_size("gz")
    count = count_x * count_y
    brick_x, brick_y, brick_z = coarse_field.shape[1:]
    smem = pl.BlockSpec(memory_space=pltpu.SMEM)
    flags, at, chosen = pl.pallas_call(
        functools.partial(plan_kernel, count_y, count_z, (brick_x, brick_y, brick_z)),
        out_shape=(
            jax.ShapeDtypeStruct((1 + 14 * SLOTS,), jnp.int32),
            jax.ShapeDtypeStruct((3,), jnp.int32),
            jax.ShapeDtypeStruct((PLANES,), jnp.int32),
        ),
        in_specs=[smem] * 3,
        out_specs=(smem, smem, smem),
        scratch_shapes=[pltpu.SMEM((count * count_z * SLOTS,), jnp.int32)],
        name="plan",
    )(corners.T, grid_slot, neighbors.T)
    anchor_y, anchor_z = at[0], at[1]

    slab = cut_slab(coarse_field, anchor_y, anchor_z)
    columns, lines, places, across = edge_matrices(brick_x + 2)
    edge_rows = lines.shape[1]
    vmem = pl.BlockSpec(memory_space=pltpu.VMEM)
    edges, planes = pl.pallas_call(
        edge_kernel,
        out_shape=(
            jax.ShapeDtypeStruct((edge_rows, LANES), jnp.float32),
            jax.ShapeDtypeStruct((PLANES * PLANE_ROWS, LANES), jnp.float32),
        ),
        in_specs=[smem] + [vmem] * 4,
        out_specs=(vmem, vmem),
        name="edge_cut",
    )(chosen, slab, fine_field, jnp.asarray(columns), jnp.asarray(lines))

    lane_mean, row_mean = mean_matrices()
    fine_out, picked = pl.pallas_call(
        functools.partial(fine_kernel, count_x, count_y, brick_x + 2),
        out_shape=(
            jax.ShapeDtypeStruct(fine_field.shape, jnp.float32),
            jax.ShapeDtypeStruct((SLOTS, MEAN_ROWS, LANES), jnp.float32),
        ),
        in_specs=[smem] + [vmem] * 8,
        out_specs=(vmem, vmem),
        scratch_shapes=[
            pltpu.VMEM((count, edge_rows, LANES), jnp.float32),
            pltpu.VMEM((count, PLANES * PLANE_ROWS, LANES), jnp.float32),
            pltpu.VMEM((SLOTS * MEAN_ROWS, LANES), jnp.float32),
            pltpu.VMEM((count, SLOTS * MEAN_ROWS, LANES), jnp.float32),
            pltpu.VMEM((3 * SLOTS * F, F * F), jnp.float32),
            pltpu.SemaphoreType.DMA((3, count)),
            pltpu.SemaphoreType.DMA((3, count)),
            pltpu.SemaphoreType.DMA((2,)),
        ],
        compiler_params=pltpu.CompilerParams(collective_id=0, has_side_effects=True),
        name="fine_step",
    )(
        flags, edges, planes, fine_field, viscosity, jnp.asarray(places), jnp.asarray(across),
        jnp.asarray(lane_mean), jnp.asarray(row_mean),
    )
    rows = picked[:, : 3 * (B // 2)].reshape(SLOTS, 3, B // 2, 2, B * B)
    rows = rows.transpose(1, 0, 3, 2, 4).reshape(3 * brick_x, B * B)
    block = 16
    coarse_out = pl.pallas_call(
        coarse_kernel,
        out_shape=jax.ShapeDtypeStruct((3 * brick_x, brick_y, brick_z), jnp.float32),
        grid_spec=pltpu.PrefetchScalarGridSpec(
            num_scalar_prefetch=1,
            grid=(3 * brick_x // block,),
            in_specs=[
                pl.BlockSpec((block, brick_y, brick_z), lambda i, at: (i, 0, 0)),
                pl.BlockSpec((block, B * B), lambda i, at: (i, 0)),
            ],
            out_specs=pl.BlockSpec((block, brick_y, brick_z), lambda i, at: (i, 0, 0)),
        ),
        name="coarse_fill",
    )(at, coarse_field.reshape(3 * brick_x, brick_y, brick_z), rows)
    return fine_out, coarse_out.reshape(coarse_field.shape)


def solution(mesh):
    in_specs = (
        P(None, "gx", "gy", "gz"),
        P(None, ("gx", "gy", "gz"), None, None),
        P(("gx", "gy", "gz"), None, None),
        P(),
        P(),
        P(),
    )
    out_specs = (P(None, ("gx", "gy", "gz"), None, None), P(None, "gx", "gy", "gz"))
    return jax.shard_map(
        on_device, mesh=mesh, in_specs=in_specs, out_specs=out_specs, check_vma=False
    )
```
